32 devices in a mesh: param: 8 (over z, x), task: 4 (over y, core).
Axes of the slice: x: 2, y: 2, z: 4, core: 2. Of those that a mesh axis runs over, the one named last changes fastest.
Arguments:
- task_ids: int32 [512], P('task'), may hold values from 0 to 511
- task_table: bfloat16 [512, 256], P('param'), may hold values from -12 to 12
- enc_in: bfloat16 [256, 512], replicated, may hold values from -0.375 to 0.375
- enc_out: bfloat16 [512, 256], replicated, may hold values from -0.25 to 0.25
- generator: bfloat16 [256, 8, 114688], P(None, None, ('param', 'task')), may hold values from -6 to 6
- gain: bfloat16 [8, 114688], P(None, ('param', 'task')), may hold values from 0.099609375 to 1.8984375
Outputs:
- adapters: bfloat16 [512, 8, 114688], P(None, None, ('param', 'task'))
The draws below stay inside these ranges and needn't reach their ends.
Inputs may be any that keep to these rules, and one draw needn't show every extreme that they name: `task_ids`: each id names a row of task_table.
All inputs are finite; a program needn't handle non-finite values.
Results may differ from the reference program's by a relative error of at most 0.00055.
The reference program's roundings to bfloat16 on the way count: a program that leaves them out, or rounds other values in their place, can miss the bound.
Values may be sent and summed in bfloat16 or wider, within the bound.
A program may use at most 192 MiB of HBM per device.

```python
import math
import jax
import jax.numpy as jnp
from jax import lax

EMB = 256
ENC = 512
LAYERS = 4
TASKS = 512
TABLE = 512
BLOCK = 114688


def draw_task_table(key, part):
    row_key, value_key = jax.random.split(jax.random.fold_in(key, 11), 2)
    scales = jnp.exp(jax.random.uniform(row_key, (TABLE, 1), jnp.float32, math.log(0.3), math.log(3.0)))
    values = jnp.clip(jax.random.normal(value_key, (TABLE, EMB), jnp.float32), -4.0, 4.0)
    return (scales * values).astype(jnp.bfloat16)


def draw_generator(key, part):
    column_key, value_key = jax.random.split(jax.random.fold_in(key, 23), 2)
    groups = 2 * LAYERS
    position = jnp.arange(BLOCK, dtype=jnp.int32).astype(jnp.float32)
    rising = jnp.exp(math.log(3.0) * position / BLOCK)
    spread = jnp.exp(jax.random.uniform(column_key, (groups, BLOCK), jnp.float32, 0.0, math.log(10.0)))
    scales = (0.05 * rising[None, :] * spread)[None, :, :]
    values = jnp.clip(jax.random.normal(value_key, (EMB, groups, BLOCK), jnp.float32), -4.0, 4.0)
    return (scales * values).astype(jnp.bfloat16)


def plant(result, own_key, low, high):
    spot = [jax.random.randint(jax.random.fold_in(own_key, axis), (), 0, length) for axis, length in enumerate(result.shape)]
    widest = result.shape.index(max(result.shape))
    neighbour = spot[:widest] + [(spot[widest] + 1) % result.shape[widest]] + spot[widest + 1:]
    return result.at[tuple(spot)].set(low).at[tuple(neighbour)].set(high)


def noise(own_key, dims, deviation, most, kind=jnp.bfloat16):
    return jnp.clip(deviation * jax.random.normal(own_key, dims, jnp.float32), -most, most).astype(kind)


def setup_inputs(seed: int = 0) -> dict:
    key_list = jax.random.split(jax.random.key(seed), 7)
    return {
        "task_ids": plant(jax.random.randint(key_list[0], (TASKS,), 0, TABLE), jax.random.fold_in(key_list[0], 1), 0, TABLE - 1).astype(jnp.int32),
        "task_table": draw_task_table(jax.random.fold_in(key_list[6], 71), 0),
        "enc_in": noise(key_list[2], (EMB, ENC), EMB ** -0.5, 0.375),
        "enc_out": noise(key_list[3], (ENC, EMB), ENC ** -0.5, 0.25),
        "generator": draw_generator(jax.random.fold_in(key_list[6], 71), 0),
        "gain": jnp.clip(1.0 + 0.18 * jax.random.normal(key_list[5], (2 * LAYERS, BLOCK), jnp.float32), 0.099609375, 1.8984375).astype(jnp.bfloat16),
    }


EPSILON = 1e-06

def encode(raw_rows, enc_in, enc_out):
    inner_act = jax.nn.gelu(jnp.dot(raw_rows, enc_in, preferred_element_type=jnp.float32)).astype(jnp.bfloat16)
    mixed_sum = raw_rows.astype(jnp.float32) + jnp.dot(inner_act, enc_out, preferred_element_type=jnp.float32)
    return mixed_sum.astype(jnp.bfloat16)

def reference(task_ids, task_table, enc_in, enc_out, generator, gain):
    raw_rows = jnp.take(task_table, task_ids.astype(jnp.int32), axis=0)
    embedded = encode(raw_rows, enc_in, enc_out)
    weight_blocks = generator.transpose(1, 0, 2)

    def normalize(operands):
        weights, gain_part = operands
        generated = jnp.dot(embedded, weights, preferred_element_type=jnp.float32)
        mean_power = lax.optimization_barrier(jnp.mean(generated * generated, axis=1, keepdims=True))
        scaled = generated * lax.rsqrt(mean_power + EPSILON) * gain_part.astype(jnp.float32)[None, :]
        return scaled.astype(jnp.bfloat16)
    stacked = lax.map(normalize, (weight_blocks, gain))
    return stacked.transpose(1, 0, 2)
```

```python
import functools

import jax
import jax.numpy as jnp
from jax import lax
from jax.experimental import pallas as pl
from jax.experimental.pallas import tpu as pltpu
from jax.sharding import PartitionSpec as P

EPSILON = 1e-06
MESH = pl.DeviceIdType.MESH
F32 = jnp.float32
BF16 = jnp.bfloat16
MIB = 1 << 20
LANES = 128
SPACE = 63 * MIB


def pieces_of(width):
    return [(start, min(LANES, width - start)) for start in range(0, width, LANES)]


def encode(raw_rows, enc_in, enc_out):
    inner_act = jax.nn.gelu(jnp.dot(raw_rows, enc_in, preferred_element_type=F32)).astype(BF16)
    mixed_sum = raw_rows.astype(F32) + jnp.dot(inner_act, enc_out, preferred_element_type=F32)
    return mixed_sum.astype(BF16)


def buffers_of(columns):
    return 1 if columns % LANES else columns // LANES


def near_factor(n):
    return max(k for k in range(1, n + 1) if n % k == 0 and k * k <= n)


def first_kernel(n_param, n_task, entries, tile, ids_hbm, table_hbm, in_hbm, out_hbm, w_hbm,
                 wt_ref, emb_ref, inv_ref,
                 *rest):
    count = buffers_of(w_hbm.shape[2])
    raw, rest = rest[:count], rest[count:]
    pour(n_param, n_task, entries, tile, ids_hbm, table_hbm, in_hbm, out_hbm, w_hbm, wt_ref, emb_ref, inv_ref, raw, *rest)


def pour(n_param, n_task, entries, tile, ids_hbm, table_hbm, in_hbm, out_hbm, w_hbm,
                 wt_ref, emb_ref, inv_ref,
                 raw, gram, ids, rows, enc_in, enc_out, coded, table, every_id, sums, part, from_near, from_far,
                 s_sem, w_sem, id_send, id_recv, row_send, row_recv, a_send, a_recv, b_send, b_recv):
    p = lax.axis_index("param")
    t = lax.axis_index("task")
    groups, blocks, emb_dim, _ = wt_ref.shape
    columns = w_hbm.shape[2]
    pieces = pieces_of(columns)
    tiles = [range(i, min(i + tile, blocks)) for i in range(0, blocks, tile)]
    low = near_factor(n_param)
    high = n_param // low
    near = low * n_task
    my_high, my_low = p // low, lax.rem(p, low)

    def along_task(k):
        return p, lax.rem(t + k, n_task)

    def along_param(k):
        return lax.rem(p + k, n_param), t

    def along_near(k):
        place = lax.rem(my_low * n_task + t + k, near)
        return my_high * low + place // n_task, lax.rem(place, n_task)

    def along_far(k):
        return lax.rem(my_high + k, high) * low + my_low, t

    barrier = pltpu.get_barrier_semaphore()
    peers = [along_param(k) for k in range(1, n_param)] + [along_near(k) for k in range(1, near)]
    for peer in peers:
        pl.semaphore_signal(barrier, inc=1, device_id=peer, device_id_type=MESH)

    small = [pltpu.make_async_copy(src, dst, s_sem.at[i]) for i, (src, dst) in enumerate(
        [(table_hbm, rows), (in_hbm, enc_in), (out_hbm, enc_out), (ids_hbm, ids)])]
    for copy in small:
        copy.start()

    def fetch(j):
        source = w_hbm if len(raw) == 1 else w_hbm.at[:, :, pieces[j][0]:pieces[j][0] + LANES]
        return pltpu.make_async_copy(source, raw[j], w_sem.at[j])

    def block(j):
        first, lane = pieces[j]
        return raw[0][:, :, first:first + lane] if len(raw) == 1 else raw[j][...]

    for j in range(len(raw)):
        fetch(j).start()
    for copy in small:
        copy.wait()
    coded[...] = encode(rows[...], enc_in[...], enc_out[...])
    table[p] = coded[...]
    every_id[t] = ids[...]
    pl.semaphore_wait(barrier, len(peers))

    def send(peer, k, src, dst, ssem, rsem):
        return pltpu.make_async_remote_copy(
            src_ref=src, dst_ref=dst, send_sem=ssem.at[k], recv_sem=rsem.at[k], device_id=peer, device_id_type=MESH)

    row_copies = [send(along_param(k), k, coded, table.at[p], row_send, row_recv) for k in range(1, n_param)]
    id_copies = [send(along_task(k), k, ids, every_id.at[t], id_send, id_recv) for k in range(1, n_task)]
    for copy in row_copies + id_copies:
        copy.start()

    def add_gram(i):
        for g in range(groups):
            w = jnp.concatenate([wt_ref[g, j][:, :pieces[j][1]] for j in tiles[i]], axis=1)
            made = lax.dot_general(w, w, (((1,), (1,)), ((), ())), preferred_element_type=F32)
            if i == 0:
                gram[g] = made
            else:
                gram[g] += made

    for i, span in enumerate(tiles):
        for j in span[:len(raw)]:
            fetch(j).wait()
        for j in span:
            wt_ref[:, j, :, :pieces[j][1]] = jnp.transpose(block(j), (1, 0, 2))
        if i:
            add_gram(i - 1)
    add_gram(len(tiles) - 1)

    for copy in row_copies + id_copies:
        copy.wait()

    rows_all = table.shape[0] * table.shape[1]
    whole = table[...].reshape(rows_all, emb_dim)
    whole_t = whole.astype(F32).T.astype(BF16)
    per = every_id.shape[2]
    labels = lax.broadcasted_iota(jnp.int32, (rows_all, per), 0)
    embedded_t = []
    for k in range(n_task):
        one_hot = jnp.where(labels == every_id[k], 1.0, 0.0).astype(BF16)
        embedded_t.append(jnp.dot(whole_t, one_hot, preferred_element_type=F32))
        emb_ref[k * per:(k + 1) * per, :] = embedded_t[k].T.astype(BF16)
    emb_t = jnp.concatenate(embedded_t, axis=1)
    emb_low = emb_t.astype(BF16)

    for g in range(groups):
        left = gram[g]
        y = None
        for _ in range(3):
            piece = left.astype(BF16)
            left = left - piece.astype(F32)
            term = jnp.dot(piece, emb_low, preferred_element_type=F32)
            y = term if y is None else y + term
        sums[g:g + 1, :] = jnp.sum(y * emb_t, axis=0, keepdims=True)

    copies = [send(along_near(k), k, sums, from_near.at[k], a_send, a_recv) for k in range(1, near)]
    for copy in copies:
        copy.start()
    for copy in copies:
        copy.wait()
    total = sums[...]
    for k in range(1, near):
        total = total + from_near[k]
    part[...] = total

    copies = [send(along_far(k), k, part, from_far.at[k], b_send, b_recv) for k in range(1, high)]
    for copy in copies:
        copy.start()
    for copy in copies:
        copy.wait()
    total = part[...]
    for k in range(1, high):
        total = total + from_far[k]
    inv_ref[...] = lax.rsqrt(total / entries + EPSILON)


def second_kernel(chunk, width, emb_ref, inv_ref, wt_ref, gain_ref, o_hbm, spread, step, sem, *outs):
    tasks = emb_ref.shape[0]
    groups, blocks, _, _ = wt_ref.shape
    pieces = pieces_of(o_hbm.shape[2])
    for g in range(groups):
        for k in range(tasks // LANES):
            row = inv_ref[g:g + 1, k * LANES:(k + 1) * LANES]
            spread[g, k * LANES:(k + 1) * LANES, :] = jnp.broadcast_to(row, (LANES, LANES)).T

    buffers = len(outs) * chunk // tasks

    def start(j, c, out):
        lanes = slice(None) if buffers == 1 else slice(pieces[j][0], pieces[j][0] + LANES)
        copy = pltpu.make_async_copy(out, o_hbm.at[c:c + chunk, :, lanes], sem.at[j % buffers, c // chunk])
        copy.start()
        return copy

    flying = []
    for n, span in enumerate(spans_of(blocks, width)):
        if n:
            pl.semaphore_signal(step, 1)
            pl.semaphore_wait(step, 1)
        for c in range(0, tasks, chunk):
            for two in (span[k:k + 2] for k in range(0, len(span), 2)):
                lanes = [pieces[j][1] for j in two]
                made = []
                for g in range(groups):
                    w = jnp.concatenate([wt_ref[g, j] for j in two], axis=1)
                    made.append(jnp.dot(emb_ref[c:c + chunk, :], w, preferred_element_type=F32))
                for q, (j, lane) in enumerate(zip(two, lanes)):
                    scaled = []
                    for g in range(groups):
                        gain = gain_ref[g:g + 1, pieces[j][0]:pieces[j][0] + lane].astype(F32)
                        part = made[g][:, q * LANES:q * LANES + lane]
                        scaled.append((part * spread[g, c:c + chunk, :lane] * gain).astype(BF16))
                    out = outs[(j % buffers) * (tasks // chunk) + c // chunk]
                    first = pieces[j][0] if buffers == 1 else 0
                    out[:, :, first:first + lane] = jnp.transpose(jnp.stack(scaled, axis=0), (1, 0, 2))
                    if buffers > 1 or j == blocks - 1:
                        flying.append(start(j, c, out))
    for copy in flying:
        copy.wait()


def spans_of(blocks, width):
    cuts = [0, 2] + list(range(2 + width, blocks - 2, width)) + [blocks - 2, blocks]
    cuts = sorted({min(max(cut, 0), blocks) for cut in cuts})
    return [list(range(a, b)) for a, b in zip(cuts, cuts[1:])]


def on_device(n_param, n_task, task_ids, task_table, enc_in, enc_out, generator, gain):
    emb_dim, groups, columns = generator.shape
    table_rows = task_table.shape[0]
    hidden = enc_in.shape[1]
    per = task_ids.shape[0]
    tasks = per * n_task
    entries = columns * n_param * n_task
    blocks = pl.cdiv(columns, LANES)
    buffers = buffers_of(columns)
    low = near_factor(n_param)
    near, high = low * n_task, n_param // low
    vmem = pl.BlockSpec(memory_space=pltpu.VMEM)
    hbm = pl.BlockSpec(memory_space=pltpu.HBM)
    dma = pltpu.SemaphoreType.DMA
    limit = SPACE - groups * emb_dim * blocks * LANES * 2 - tasks * emb_dim * 2 - groups * tasks * 4
    wt, embedded, inverse = pl.pallas_call(
        functools.partial(first_kernel, n_param, n_task, entries, 4),
        out_shape=(
            pltpu.VMEM((groups, blocks, emb_dim, LANES), BF16),
            pltpu.VMEM((tasks, emb_dim), BF16),
            pltpu.VMEM((groups, tasks), F32),
        ),
        in_specs=[hbm] * 5,
        out_specs=(vmem, vmem, vmem),
        scratch_shapes=[
            *[pltpu.VMEM((emb_dim, groups, columns // buffers), BF16) for _ in range(buffers)],
            pltpu.VMEM((groups, emb_dim, emb_dim), F32),
            pltpu.VMEM((1, per), jnp.int32),
            pltpu.VMEM((table_rows, emb_dim), BF16),
            pltpu.VMEM((emb_dim, hidden), BF16),
            pltpu.VMEM((hidden, emb_dim), BF16),
            pltpu.VMEM((table_rows, emb_dim), BF16),
            pltpu.VMEM((n_param, table_rows, emb_dim), BF16),
            pltpu.VMEM((n_task, 1, per), jnp.int32),
            pltpu.VMEM((groups, tasks), F32),
            pltpu.VMEM((groups, tasks), F32),
            pltpu.VMEM((near, groups, tasks), F32),
            pltpu.VMEM((high, groups, tasks), F32),
            dma((4,)),
            dma((buffers,)),
            dma((n_task,)), dma((n_task,)),
            dma((n_param,)), dma((n_param,)),
            dma((near,)), dma((near,)),
            dma((high,)), dma((high,)),
        ],
        compiler_params=pltpu.CompilerParams(
            collective_id=0, has_side_effects=True, vmem_limit_bytes=limit),
        name="gather_power",
    )(task_ids.reshape(1, per), task_table, enc_in, enc_out, generator)

    chunk = min(tasks, 512)
    return pl.pallas_call(
        functools.partial(second_kernel, chunk, 4),
        out_shape=jax.ShapeDtypeStruct((tasks, groups, columns), BF16),
        in_specs=[vmem] * 4,
        out_specs=hbm,
        scratch_shapes=[
            pltpu.VMEM((groups, tasks, LANES), F32),
            pltpu.SemaphoreType.REGULAR,
            dma((buffers, tasks // chunk)),
            *[pltpu.VMEM((chunk, groups, columns // buffers), BF16) for _ in range(buffers * (tasks // chunk))],
        ],
        compiler_params=pltpu.CompilerParams(vmem_limit_bytes=tasks * groups * LANES * (4 + 2 * blocks) + (3 if buffers > 1 else 12) * MIB),
        name="generate_scale",
    )(embedded, inverse, wt, gain)


def solution(mesh):
    placed = (
        P("task"),
        P("param", None),
        P(),
        P(),
        P(None, None, ("param", "task")),
        P(None, ("param", "task")),
    )
    return jax.shard_map(
        functools.partial(on_device, mesh.shape["param"], mesh.shape["task"]),
        mesh=mesh,
        in_specs=placed,
        out_specs=P(None, None, ("param", "task")),
        check_vma=False,
    )
```

```python
import functools

import jax
import jax.numpy as jnp
from jax import lax
from jax.experimental import pallas as pl
from jax.experimental.pallas import tpu as pltpu
from jax.sharding import PartitionSpec as P

EPSILON = 1e-06
MESH = pl.DeviceIdType.MESH
F32 = jnp.float32
BF16 = jnp.bfloat16
MIB = 1 << 20
LANES = 128
TILE = 512
ROWS = 32
STAGES = 4
PITCH = 9
AHEAD = 2
HALF = 2
SPACE = 63 * MIB


def pieces_of(width):
    return [(start, min(LANES, width - start)) for start in range(0, width, LANES)]


def encode(raw_rows, enc_in, enc_out):
    inner_act = jax.nn.gelu(jnp.dot(raw_rows, enc_in, preferred_element_type=F32)).astype(BF16)
    mixed_sum = raw_rows.astype(F32) + jnp.dot(inner_act, enc_out, preferred_element_type=F32)
    return mixed_sum.astype(BF16)


def buffers_of(columns):
    return 1 if columns % LANES else columns // LANES


def tiles_of(columns):
    return 1 if columns % TILE else columns // TILE


def near_factor(n):
    return max(k for k in range(1, n + 1) if n % k == 0 and k * k <= n)


def first_kernel(n_param, n_task, entries, ids_hbm, table_hbm, in_hbm, out_hbm, w_hbm,
                 even_ref, odd_ref, emb_ref, inv_ref,
                 raw, stage, gram, ids, rows, enc_in, enc_out, coded, table, every_id, sums, part, from_near, from_far,
                 s_sem, w_sem, id_send, id_recv, row_send, row_recv, a_send, a_recv, b_send, b_recv):
    p = lax.axis_index("param")
    t = lax.axis_index("task")
    _, groups, blocks, emb_dim, _ = even_ref.shape
    columns = w_hbm.shape[2]
    tiles = tiles_of(columns)
    pieces = pieces_of(columns // tiles)
    low = near_factor(n_param)
    high = n_param // low
    near = low * n_task
    my_high, my_low = p // low, lax.rem(p, low)

    def along_task(k):
        return p, lax.rem(t + k, n_task)

    def along_param(k):
        return lax.rem(p + k, n_param), t

    def along_near(k):
        place = lax.rem(my_low * n_task + t + k, near)
        return my_high * low + place // n_task, lax.rem(place, n_task)

    def along_far(k):
        return lax.rem(my_high + k, high) * low + my_low, t

    barrier = pltpu.get_barrier_semaphore()
    peers = [along_param(k) for k in range(1, n_param)] + [along_near(k) for k in range(1, near)]
    for peer in peers:
        pl.semaphore_signal(barrier, inc=1, device_id=peer, device_id_type=MESH)

    small = [pltpu.make_async_copy(src, dst, s_sem.at[i]) for i, (src, dst) in enumerate(
        [(table_hbm, rows), (in_hbm, enc_in), (out_hbm, enc_out), (ids_hbm, ids)])]
    for copy in small:
        copy.start()

    def fetches(i):
        if tiles == 1:
            return [pltpu.make_async_copy(w_hbm, raw.at[0, 0], w_sem.at[0, 0])]
        return [pltpu.make_async_copy(
            w_hbm.at[:, :, pl.ds(pl.multiple_of((i * blocks + q) * LANES, LANES), LANES)], raw.at[i, q], w_sem.at[i, q])
            for q in range(blocks)]

    def begin(i):
        for copy in fetches(i):
            copy.start()

    for i in range(min(AHEAD, tiles)):
        begin(i)
    for copy in small:
        copy.wait()
    coded[...] = encode(rows[...], enc_in[...], enc_out[...])
    table[p] = coded[...]
    every_id[t] = ids[...]
    pl.semaphore_wait(barrier, len(peers))

    def send(peer, k, src, dst, ssem, rsem):
        return pltpu.make_async_remote_copy(
            src_ref=src, dst_ref=dst, send_sem=ssem.at[k], recv_sem=rsem.at[k], device_id=peer, device_id_type=MESH)

    row_copies = [send(along_param(k), k, coded, table.at[p], row_send, row_recv) for k in range(1, n_param)]
    id_copies = [send(along_task(k), k, ids, every_id.at[t], id_send, id_recv) for k in range(1, n_task)]
    for copy in row_copies + id_copies:
        copy.start()

    def ready(i):
        for copy in fetches(i):
            copy.wait()
        if i + AHEAD < tiles:
            begin(i + AHEAD)

    def reorder(i, w_ref, k, some):
        for q, (first, lane) in some:
            for n, r in enumerate(range(0, emb_dim, ROWS)):
                rows = pl.ds(r, ROWS)
                part = raw[0, 0, rows, :, first:first + lane] if tiles == 1 else raw[i, q, rows]
                wide = part.astype(F32)
                spot = (n + q * (emb_dim // ROWS)) % STAGES * ROWS * PITCH
                for e in range(ROWS):
                    stage[spot + e * PITCH:spot + e * PITCH + groups, :lane] = wide[e]
                for g in range(groups):
                    w_ref[k, g, q, rows, :lane] = stage[pl.ds(spot + g, ROWS, stride=PITCH), :][:, :lane].astype(BF16)

    def add_gram(w_ref, k, some):
        for g in range(groups):
            w = jnp.concatenate([w_ref[k, g, q][:, :lane] for q, (_, lane) in some], axis=1)
            gram[g] += lax.dot_general(w, w, (((1,), (1,)), ((), ())), preferred_element_type=F32)

    gram[...] = jnp.zeros_like(gram)
    steps = list(enumerate(pieces))
    for i in range(tiles):
        ready(i)
        w_ref = odd_ref if i % 2 else even_ref
        for n in range(0, blocks, HALF):
            reorder(i, w_ref, i // 2, steps[n:n + HALF])
            add_gram(w_ref, i // 2, steps[n:n + HALF])

    for copy in row_copies + id_copies:
        copy.wait()

    rows_all = table.shape[0] * table.shape[1]
    whole = table[...].reshape(rows_all, emb_dim)
    whole_t = whole.astype(F32).T.astype(BF16)
    per = every_id.shape[2]
    labels = lax.broadcasted_iota(jnp.int32, (rows_all, per), 0)
    embedded_t = []
    for k in range(n_task):
        one_hot = jnp.where(labels == every_id[k], 1.0, 0.0).astype(BF16)
        embedded_t.append(jnp.dot(whole_t, one_hot, preferred_element_type=F32))
        emb_ref[k * per:(k + 1) * per, :] = embedded_t[k].T.astype(BF16)
    emb_t = jnp.concatenate(embedded_t, axis=1)
    emb_low = emb_t.astype(BF16)

    for g in range(groups):
        left = gram[g]
        y = None
        for _ in range(2):
            piece = left.astype(BF16)
            left = left - piece.astype(F32)
            term = jnp.dot(piece, emb_low, preferred_element_type=F32)
            y = term if y is None else y + term
        sums[g:g + 1, :] = jnp.sum(y * emb_t, axis=0, keepdims=True)

    copies = [send(along_near(k), k, sums, from_near.at[k], a_send, a_recv) for k in range(1, near)]
    for copy in copies:
        copy.start()
    for copy in copies:
        copy.wait()
    total = sums[...]
    for k in range(1, near):
        total = total + from_near[k]
    part[...] = total

    copies = [send(along_far(k), k, part, from_far.at[k], b_send, b_recv) for k in range(1, high)]
    for copy in copies:
        copy.start()
    for copy in copies:
        copy.wait()
    total = part[...]
    for k in range(1, high):
        total = total + from_far[k]
    inv_ref[...] = lax.rsqrt(total / entries + EPSILON)


def second_kernel(chunk, width, emb_ref, inv_ref, even_ref, odd_ref, gain_ref, o_hbm, spread, step, sem, *outs):
    tasks = emb_ref.shape[0]
    _, groups, in_tile, _, _ = even_ref.shape
    pieces = pieces_of(o_hbm.shape[2])
    blocks = len(pieces)
    for g in range(groups):
        for k in range(tasks // LANES):
            row = inv_ref[g:g + 1, k * LANES:(k + 1) * LANES]
            spread[g, k * LANES:(k + 1) * LANES, :] = jnp.broadcast_to(row, (LANES, LANES)).T

    buffers = len(outs) * chunk // tasks

    def weights(j, g):
        i = j // in_tile
        return (odd_ref if i % 2 else even_ref)[i // 2, g, j % in_tile]

    def start(j, c, out):
        lanes = slice(None) if buffers == 1 else slice(pieces[j][0], pieces[j][0] + LANES)
        copy = pltpu.make_async_copy(out, o_hbm.at[c:c + chunk, :, lanes], sem.at[j % buffers, c // chunk])
        copy.start()
        return copy

    flying = []
    for n, span in enumerate(spans_of(blocks, width)):
        if n:
            pl.semaphore_signal(step, 1)
            pl.semaphore_wait(step, 1)
        for c in range(0, tasks, chunk):
            for two in (span[k:k + 2] for k in range(0, len(span), 2)):
                lanes = [pieces[j][1] for j in two]
                made = []
                for g in range(groups):
                    w = jnp.concatenate([weights(j, g) for j in two], axis=1)
                    made.append(jnp.dot(emb_ref[c:c + chunk, :], w, preferred_element_type=F32))
                for q, (j, lane) in enumerate(zip(two, lanes)):
                    scaled = []
                    for g in range(groups):
                        gain = gain_ref[g:g + 1, pieces[j][0]:pieces[j][0] + lane].astype(F32)
                        part = made[g][:, q * LANES:q * LANES + lane]
                        scaled.append((part * spread[g, c:c + chunk, :lane] * gain).astype(BF16))
                    out = outs[(j % buffers) * (tasks // chunk) + c // chunk]
                    first = pieces[j][0] if buffers == 1 else 0
                    out[:, :, first:first + lane] = jnp.transpose(jnp.stack(scaled, axis=0), (1, 0, 2))
                    if buffers > 1 or j == blocks - 1:
                        flying.append(start(j, c, out))
    for copy in flying:
        copy.wait()


def spans_of(blocks, width):
    cuts = [0, 2] + list(range(2 + width, blocks - 2, width)) + [blocks - 2, blocks]
    cuts = sorted({min(max(cut, 0), blocks) for cut in cuts})
    return [list(range(a, b)) for a, b in zip(cuts, cuts[1:])]


def on_device(n_param, n_task, task_ids, task_table, enc_in, enc_out, generator, gain):
    emb_dim, groups, columns = generator.shape
    table_rows = task_table.shape[0]
    hidden = enc_in.shape[1]
    per = task_ids.shape[0]
    tasks = per * n_task
    entries = columns * n_param * n_task
    blocks = pl.cdiv(columns, LANES)
    buffers = buffers_of(columns)
    tiles = tiles_of(columns)
    in_tile = blocks // tiles
    low = near_factor(n_param)
    near, high = low * n_task, n_param // low
    vmem = pl.BlockSpec(memory_space=pltpu.VMEM)
    hbm = pl.BlockSpec(memory_space=pltpu.HBM)
    dma = pltpu.SemaphoreType.DMA
    limit = SPACE - groups * emb_dim * max(blocks, 2 * in_tile) * LANES * 2 - tasks * emb_dim * 2 - groups * tasks * 4
    even, odd, embedded, inverse = pl.pallas_call(
        functools.partial(first_kernel, n_param, n_task, entries),
        out_shape=(
            pltpu.VMEM((pl.cdiv(tiles, 2), groups, in_tile, emb_dim, LANES), BF16),
            pltpu.VMEM((max(tiles // 2, 1), groups, in_tile, emb_dim, LANES), BF16),
            pltpu.VMEM((tasks, emb_dim), BF16),
            pltpu.VMEM((groups, tasks), F32),
        ),
        in_specs=[hbm] * 5,
        out_specs=(vmem, vmem, vmem, vmem),
        scratch_shapes=[
            pltpu.VMEM((tiles, in_tile, emb_dim, groups, LANES) if tiles > 1 else (1, 1, emb_dim, groups, columns), BF16),
            pltpu.VMEM((STAGES * ROWS * PITCH, LANES), F32),
            pltpu.VMEM((groups, emb_dim, emb_dim), F32),
            pltpu.VMEM((1, per), jnp.int32),
            pltpu.VMEM((table_rows, emb_dim), BF16),
            pltpu.VMEM((emb_dim, hidden), BF16),
            pltpu.VMEM((hidden, emb_dim), BF16),
            pltpu.VMEM((table_rows, emb_dim), BF16),
            pltpu.VMEM((n_param, table_rows, emb_dim), BF16),
            pltpu.VMEM((n_task, 1, per), jnp.int32),
            pltpu.VMEM((groups, tasks), F32),
            pltpu.VMEM((groups, tasks), F32),
            pltpu.VMEM((near, groups, tasks), F32),
            pltpu.VMEM((high, groups, tasks), F32),
            dma((4,)),
            dma((tiles, in_tile)),
            dma((n_task,)), dma((n_task,)),
            dma((n_param,)), dma((n_param,)),
            dma((near,)), dma((near,)),
            dma((high,)), dma((high,)),
        ],
        compiler_params=pltpu.CompilerParams(
            collective_id=0, has_side_effects=True, vmem_limit_bytes=limit),
        name="gather_power",
    )(task_ids.reshape(1, per), task_table, enc_in, enc_out, generator)

    chunk = min(tasks, 512)
    return pl.pallas_call(
        functools.partial(second_kernel, chunk, 4),
        out_shape=jax.ShapeDtypeStruct((tasks, groups, columns), BF16),
        in_specs=[vmem] * 5,
        out_specs=hbm,
        scratch_shapes=[
            pltpu.VMEM((groups, tasks, LANES), F32),
            pltpu.SemaphoreType.REGULAR,
            dma((buffers, tasks // chunk)),
            *[pltpu.VMEM((chunk, groups, columns // buffers), BF16) for _ in range(buffers * (tasks // chunk))],
        ],
        compiler_params=pltpu.CompilerParams(vmem_limit_bytes=tasks * groups * LANES * (4 + 2 * blocks) + (3 if buffers > 1 else 12) * MIB),
        name="generate_scale",
    )(embedded, inverse, even, odd, gain)


def solution(mesh):
    placed = (
        P("task"),
        P("param", None),
        P(),
        P(),
        P(None, None, ("param", "task")),
        P(None, ("param", "task")),
    )
    return jax.shard_map(
        functools.partial(on_device, mesh.shape["param"], mesh.shape["task"]),
        mesh=mesh,
        in_specs=placed,
        out_specs=P(None, None, ("param", "task")),
        check_vma=False,
    )
```

```python
import functools

import jax
import jax.numpy as jnp
from jax import lax
from jax.experimental import pallas as pl
from jax.experimental.pallas import tpu as pltpu
from jax.sharding import PartitionSpec as P

EPSILON = 1e-06
MESH = pl.DeviceIdType.MESH
F32 = jnp.float32
BF16 = jnp.bfloat16
MIB = 1 << 20
LANES = 128
TILE = 512
ROWS = 32
STAGES = 4
PITCH = 9
AHEAD = 2
SPLIT = 2
EARLY = 512
HALF = 2
SPACE = 63 * MIB


def pieces_of(width):
    return [(start, min(LANES, width - start)) for start in range(0, width, LANES)]


def encode(raw_rows, enc_in, enc_out):
    inner_act = jax.nn.gelu(jnp.dot(raw_rows, enc_in, preferred_element_type=F32)).astype(BF16)
    mixed_sum = raw_rows.astype(F32) + jnp.dot(inner_act, enc_out, preferred_element_type=F32)
    return mixed_sum.astype(BF16)


def buffers_of(columns):
    return 1 if columns % LANES else columns // LANES


def tiles_of(columns):
    return 1 if columns % TILE else columns // TILE


def near_factor(n):
    return max(k for k in range(1, n + 1) if n % k == 0 and k * k <= n)


def first_kernel(n_param, n_task, entries, ids_hbm, table_hbm, in_hbm, out_hbm, w_hbm,
                 even_ref, odd_ref, emb_ref, inv_ref,
                 raw, stage, gram, ids, rows, enc_in, enc_out, coded, table, every_id, turned, sums, part, from_near, from_far,
                 s_sem, w_sem, id_send, id_recv, row_send, row_recv, a_send, a_recv, b_send, b_recv):
    p = lax.axis_index("param")
    t = lax.axis_index("task")
    _, groups, blocks, emb_dim, _ = even_ref.shape
    columns = w_hbm.shape[2]
    tiles = tiles_of(columns)
    pieces = pieces_of(columns // tiles)
    low = near_factor(n_param)
    high = n_param // low
    near = low * n_task
    my_high, my_low = p // low, lax.rem(p, low)

    def along_task(k):
        return p, lax.rem(t + k, n_task)

    def along_param(k):
        return lax.rem(p + k, n_param), t

    def along_near(k):
        place = lax.rem(my_low * n_task + t + k, near)
        return my_high * low + place // n_task, lax.rem(place, n_task)

    def along_far(k):
        return lax.rem(my_high + k, high) * low + my_low, t

    barrier = pltpu.get_barrier_semaphore()
    peers = [along_param(k) for k in range(1, n_param)] + [along_near(k) for k in range(1, near)]
    for peer in peers:
        pl.semaphore_signal(barrier, inc=1, device_id=peer, device_id_type=MESH)

    small = [pltpu.make_async_copy(src, dst, s_sem.at[i]) for i, (src, dst) in enumerate(
        [(table_hbm, rows), (in_hbm, enc_in), (out_hbm, enc_out), (ids_hbm, ids)])]
    for copy in small:
        copy.start()

    def fetches(i):
        if tiles == 1:
            return [pltpu.make_async_copy(w_hbm, raw.at[0, 0], w_sem.at[0, 0])]
        return [pltpu.make_async_copy(
            w_hbm.at[:, :, pl.ds(pl.multiple_of((i * blocks + q) * LANES, LANES), LANES)], raw.at[i, q], w_sem.at[i, q])
            for q in range(blocks)]

    def begin(i):
        for copy in fetches(i):
            copy.start()

    begin(0)
    for copy in small:
        copy.wait()
    for i in range(1, min(AHEAD, tiles)):
        begin(i)
    coded[...] = encode(rows[...], enc_in[...], enc_out[...])
    table[p] = coded[...]
    every_id[t] = ids[...]
    pl.semaphore_wait(barrier, len(peers))

    def send(peer, k, src, dst, ssem, rsem):
        return pltpu.make_async_remote_copy(
            src_ref=src, dst_ref=dst, send_sem=ssem.at[k], recv_sem=rsem.at[k], device_id=peer, device_id_type=MESH)

    row_copies = [send(along_param(k), k, coded, table.at[p], row_send, row_recv) for k in range(1, n_param)]
    id_copies = [send(along_task(k), k, ids, every_id.at[t], id_send, id_recv) for k in range(1, n_task)]
    for copy in row_copies + id_copies:
        copy.start()

    def ready(i):
        for copy in fetches(i):
            copy.wait()
        if i + AHEAD < tiles:
            begin(i + AHEAD)

    def reorder(i, w_ref, k, some):
        for q, (first, lane) in some:
            for n, r in enumerate(range(0, emb_dim, ROWS)):
                rows = pl.ds(r, ROWS)
                part = raw[0, 0, rows, :, first:first + lane] if tiles == 1 else raw[i, q, rows]
                wide = part.astype(F32)
                spot = (n + q * (emb_dim // ROWS)) % STAGES * ROWS * PITCH
                for e in range(ROWS):
                    stage[spot + e * PITCH:spot + e * PITCH + groups, :lane] = wide[e]
                for g in range(groups):
                    w_ref[k, g, q, rows, :lane] = stage[pl.ds(spot + g, ROWS, stride=PITCH), :][:, :lane].astype(BF16)

    def add_gram(w_ref, k, some):
        for g in range(groups):
            w = jnp.concatenate([w_ref[k, g, q][:, :lane] for q, (_, lane) in some], axis=1)
            gram[g] += lax.dot_general(w, w, (((1,), (1,)), ((), ())), preferred_element_type=F32)

    gram[...] = jnp.zeros_like(gram)
    steps = list(enumerate(pieces))
    def embed():
        for copy in row_copies + id_copies:
            copy.wait()

        rows_all = table.shape[0] * table.shape[1]
        whole = table[...].reshape(rows_all, emb_dim)
        whole_t = whole.astype(F32).T.astype(BF16)
        per = every_id.shape[2]
        labels = lax.broadcasted_iota(jnp.int32, (rows_all, per), 0)
        embedded_t = []
        for k in range(n_task):
            one_hot = jnp.where(labels == every_id[k], 1.0, 0.0).astype(BF16)
            embedded_t.append(jnp.dot(whole_t, one_hot, preferred_element_type=F32))
            emb_ref[k * per:(k + 1) * per, :] = embedded_t[k].T.astype(BF16)
        emb_t = jnp.concatenate(embedded_t, axis=1)
        turned[...] = emb_t

    for i in range(tiles):
        ready(i)
        w_ref = odd_ref if i % 2 else even_ref
        for n in range(0, blocks, HALF):
            reorder(i, w_ref, i // 2, steps[n:n + HALF])
            add_gram(w_ref, i // 2, steps[n:n + HALF])

    embed()
    count = turned.shape[1]
    width = max(count // SPLIT, LANES)
    halves = [slice(h, h + width) for h in range(0, count, width)]
    first_trip, second_trip = [], []
    for h, lanes in enumerate(halves):
        emb_t = turned[:, lanes]
        emb_low = emb_t.astype(BF16)
        for g in range(groups):
            left = gram[g]
            y = None
            for _ in range(2):
                piece = left.astype(BF16)
                left = left - piece.astype(F32)
                term = jnp.dot(piece, emb_low, preferred_element_type=F32)
                y = term if y is None else y + term
            sums[g:g + 1, lanes] = jnp.sum(y * emb_t, axis=0, keepdims=True)
        first_trip.append([send(along_near(k), (h, k), sums.at[:, lanes], from_near.at[k, :, lanes], a_send, a_recv)
                           for k in range(1, near)])
        for copy in first_trip[h]:
            copy.start()

    for h, lanes in enumerate(halves):
        for copy in first_trip[h]:
            copy.wait()
        total = sums[:, lanes]
        for k in range(1, near):
            total = total + from_near[k, :, lanes]
        part[:, lanes] = total
        second_trip.append([send(along_far(k), (h, k), part.at[:, lanes], from_far.at[k, :, lanes], b_send, b_recv)
                            for k in range(1, high)])
        for copy in second_trip[h]:
            copy.start()

    for h, lanes in enumerate(halves):
        for copy in second_trip[h]:
            copy.wait()
        total = part[:, lanes]
        for k in range(1, high):
            total = total + from_far[k, :, lanes]
        inv_ref[:, lanes] = lax.rsqrt(total / entries + EPSILON)


def second_kernel(keys, width, emb_ref, inv_ref, even_ref, odd_ref, gain_ref, o_hbm, spread, step, sem, *outs):
    tasks = emb_ref.shape[0]
    _, groups, in_tile, _, _ = even_ref.shape
    pieces = pieces_of(o_hbm.shape[2])
    blocks = len(pieces)
    buffers = len({j for j, _, _ in keys})

    def weights(j, g):
        i = j // in_tile
        return (odd_ref if i % 2 else even_ref)[i // 2, g, j % in_tile]

    def widen(c, count):
        for g in range(groups):
            for k in range(c, c + count, LANES):
                row = inv_ref[g:g + 1, k:k + LANES]
                spread[g, k:k + LANES, :] = jnp.broadcast_to(row, (LANES, LANES)).T

    def make(two, c, count):
        made = []
        for g in range(groups):
            w = jnp.concatenate([weights(j, g) for j in two], axis=1)
            made.append(jnp.dot(emb_ref[c:c + count, :], w, preferred_element_type=F32))
        for q, j in enumerate(two):
            lo, lane = pieces[j]
            scaled = []
            for g in range(groups):
                gain = gain_ref[g:g + 1, lo:lo + lane].astype(F32)
                part = made[g][:, q * LANES:q * LANES + lane]
                scaled.append((part * spread[g, c:c + count, :lane] * gain).astype(BF16))
            n = keys.index((j % buffers, c, count))
            first = lo if buffers == 1 else 0
            outs[n][:, :, first:first + lane] = jnp.transpose(jnp.stack(scaled, axis=0), (1, 0, 2))
            if buffers > 1 or j == blocks - 1:
                lanes = slice(None) if buffers == 1 else slice(lo, lo + LANES)
                copy = pltpu.make_async_copy(outs[n], o_hbm.at[c:c + count, :, lanes], sem.at[n])
                copy.start()
                flying.append(copy)

    flying = []
    spans = spans_of(blocks, width) if buffers > 1 else [list(range(blocks))]
    for n, span in enumerate(spans):
        for c, count in cuts_of(tasks, buffers > 1 and n == 0):
            if n == 0:
                widen(c, count)
            for k in range(0, len(span), 2):
                make(span[k:k + 2], c, count)
            pl.semaphore_signal(step, 1)
            pl.semaphore_wait(step, 1)
    for copy in flying:
        copy.wait()


def cuts_of(tasks, fine):
    size = min(tasks, 512)
    cuts = [(c, size) for c in range(0, tasks, size)]
    return [(0, EARLY), (EARLY, size - EARLY)] + cuts[1:] if fine and size > EARLY else cuts


def spans_of(blocks, width):
    cuts = [0, 2] + list(range(2 + width, blocks - 2, width)) + [blocks - 2, blocks]
    cuts = sorted({min(max(cut, 0), blocks) for cut in cuts})
    return [list(range(a, b)) for a, b in zip(cuts, cuts[1:])]


def on_device(n_param, n_task, task_ids, task_table, enc_in, enc_out, generator, gain):
    emb_dim, groups, columns = generator.shape
    table_rows = task_table.shape[0]
    hidden = enc_in.shape[1]
    per = task_ids.shape[0]
    tasks = per * n_task
    entries = columns * n_param * n_task
    blocks = pl.cdiv(columns, LANES)
    buffers = buffers_of(columns)
    tiles = tiles_of(columns)
    in_tile = blocks // tiles
    low = near_factor(n_param)
    near, high = low * n_task, n_param // low
    vmem = pl.BlockSpec(memory_space=pltpu.VMEM)
    hbm = pl.BlockSpec(memory_space=pltpu.HBM)
    dma = pltpu.SemaphoreType.DMA
    limit = SPACE - groups * emb_dim * max(blocks, 2 * in_tile) * LANES * 2 - tasks * emb_dim * 2 - groups * tasks * 4
    even, odd, embedded, inverse = pl.pallas_call(
        functools.partial(first_kernel, n_param, n_task, entries),
        out_shape=(
            pltpu.VMEM((pl.cdiv(tiles, 2), groups, in_tile, emb_dim, LANES), BF16),
            pltpu.VMEM((max(tiles // 2, 1), groups, in_tile, emb_dim, LANES), BF16),
            pltpu.VMEM((tasks, emb_dim), BF16),
            pltpu.VMEM((groups, tasks), F32),
        ),
        in_specs=[hbm] * 5,
        out_specs=(vmem, vmem, vmem, vmem),
        scratch_shapes=[
            pltpu.VMEM((tiles, in_tile, emb_dim, groups, LANES) if tiles > 1 else (1, 1, emb_dim, groups, columns), BF16),
            pltpu.VMEM((STAGES * ROWS * PITCH, LANES), F32),
            pltpu.VMEM((groups, emb_dim, emb_dim), F32),
            pltpu.VMEM((1, per), jnp.int32),
            pltpu.VMEM((table_rows, emb_dim), BF16),
            pltpu.VMEM((emb_dim, hidden), BF16),
            pltpu.VMEM((hidden, emb_dim), BF16),
            pltpu.VMEM((table_rows, emb_dim), BF16),
            pltpu.VMEM((n_param, table_rows, emb_dim), BF16),
            pltpu.VMEM((n_task, 1, per), jnp.int32),
            pltpu.VMEM((emb_dim, tasks), F32),
            pltpu.VMEM((groups, tasks), F32),
            pltpu.VMEM((groups, tasks), F32),
            pltpu.VMEM((near, groups, tasks), F32),
            pltpu.VMEM((high, groups, tasks), F32),
            dma((4,)),
            dma((tiles, in_tile)),
            dma((n_task,)), dma((n_task,)),
            dma((n_param,)), dma((n_param,)),
            dma((SPLIT, near)), dma((SPLIT, near)),
            dma((SPLIT, high)), dma((SPLIT, high)),
        ],
        compiler_params=pltpu.CompilerParams(
            collective_id=0, has_side_effects=True, vmem_limit_bytes=limit),
        name="gather_power",
    )(task_ids.reshape(1, per), task_table, enc_in, enc_out, generator)

    keys = [(j, c, n) for j in range(buffers) for c, n in cuts_of(tasks, buffers > 1 and j < 2)]
    return pl.pallas_call(
        functools.partial(second_kernel, keys, 4),
        out_shape=jax.ShapeDtypeStruct((tasks, groups, columns), BF16),
        in_specs=[vmem] * 5,
        out_specs=hbm,
        scratch_shapes=[
            pltpu.VMEM((groups, tasks, LANES), F32),
            pltpu.SemaphoreType.REGULAR,
            dma((len(keys),)),
            *[pltpu.VMEM((n, groups, columns // buffers), BF16) for _, _, n in keys],
        ],
        compiler_params=pltpu.CompilerParams(vmem_limit_bytes=tasks * groups * LANES * (4 + 2 * blocks) + (3 if buffers > 1 else 12) * MIB),
        name="generate_scale",
    )(embedded, inverse, even, odd, gain)


def solution(mesh):
    placed = (
        P("task"),
        P("param", None),
        P(),
        P(),
        P(None, None, ("param", "task")),
        P(None, ("param", "task")),
    )
    return jax.shard_map(
        functools.partial(on_device, mesh.shape["param"], mesh.shape["task"]),
        mesh=mesh,
        in_specs=placed,
        out_specs=P(None, None, ("param", "task")),
        check_vma=False,
    )
```

```python
import functools

import jax
import jax.numpy as jnp
from jax import lax
from jax.experimental import pallas as pl
from jax.experimental.pallas import tpu as pltpu
from jax.sharding import PartitionSpec as P

EPSILON = 1e-06
MESH = pl.DeviceIdType.MESH
F32 = jnp.float32
BF16 = jnp.bfloat16
MIB = 1 << 20
LANES = 128
TILE = 512
ROWS = 32
STAGES = 16
PITCH = 9
AHEAD = 2
SPLIT = 2
EARLY = 512
HALF = 2
SPACE = 63 * MIB


def pieces_of(width):
    return [(start, min(LANES, width - start)) for start in range(0, width, LANES)]


def encode(raw_rows, enc_in, enc_out):
    inner_act = jax.nn.gelu(jnp.dot(raw_rows, enc_in, preferred_element_type=F32)).astype(BF16)
    mixed_sum = raw_rows.astype(F32) + jnp.dot(inner_act, enc_out, preferred_element_type=F32)
    return mixed_sum.astype(BF16)


def buffers_of(columns):
    return 1 if columns % LANES else columns // LANES


def tiles_of(columns):
    return 1 if columns % TILE else columns // TILE


def near_factor(n):
    return max(k for k in range(1, n + 1) if n % k == 0 and k * k <= n)


def first_kernel(n_param, n_task, entries, ids_hbm, table_hbm, in_hbm, out_hbm, w_hbm,
                 even_ref, odd_ref, emb_ref, inv_ref,
                 raw, stage, gram, ids, rows, enc_in, enc_out, coded, table, every_id, turned, sums, part, from_near, from_far,
                 s_sem, w_sem, id_send, id_recv, row_send, row_recv, a_send, a_recv, b_send, b_recv):
    p = lax.axis_index("param")
    t = lax.axis_index("task")
    _, groups, blocks, emb_dim, _ = even_ref.shape
    columns = w_hbm.shape[2]
    tiles = tiles_of(columns)
    pieces = pieces_of(columns // tiles)
    low = near_factor(n_param)
    high = n_param // low
    near = low * n_task
    my_high, my_low = p // low, lax.rem(p, low)

    def along_task(k):
        return p, lax.rem(t + k, n_task)

    def along_param(k):
        return lax.rem(p + k, n_param), t

    def along_near(k):
        place = lax.rem(my_low * n_task + t + k, near)
        return my_high * low + place // n_task, lax.rem(place, n_task)

    def along_far(k):
        return lax.rem(my_high + k, high) * low + my_low, t

    barrier = pltpu.get_barrier_semaphore()
    peers = [along_param(k) for k in range(1, n_param)] + [along_near(k) for k in range(1, near)]
    for peer in peers:
        pl.semaphore_signal(barrier, inc=1, device_id=peer, device_id_type=MESH)

    small = [pltpu.make_async_copy(src, dst, s_sem.at[i]) for i, (src, dst) in enumerate(
        [(table_hbm, rows), (in_hbm, enc_in), (out_hbm, enc_out), (ids_hbm, ids)])]
    for copy in small:
        copy.start()

    def fetches(i):
        if tiles == 1:
            return [pltpu.make_async_copy(w_hbm, raw.at[0, 0], w_sem.at[0, 0])]
        return [pltpu.make_async_copy(
            w_hbm.at[:, :, pl.ds(pl.multiple_of((i * blocks + q) * LANES, LANES), LANES)], raw.at[i, q], w_sem.at[i, q])
            for q in range(blocks)]

    def begin(i):
        for copy in fetches(i):
            copy.start()

    begin(0)
    for copy in small:
        copy.wait()
    for i in range(1, min(AHEAD, tiles)):
        begin(i)
    coded[...] = encode(rows[...], enc_in[...], enc_out[...])
    table[p] = coded[...]
    every_id[t] = ids[...]
    pl.semaphore_wait(barrier, len(peers))

    def send(peer, k, src, dst, ssem, rsem):
        return pltpu.make_async_remote_copy(
            src_ref=src, dst_ref=dst, send_sem=ssem.at[k], recv_sem=rsem.at[k], device_id=peer, device_id_type=MESH)

    row_copies = [send(along_param(k), k, coded, table.at[p], row_send, row_recv) for k in range(1, n_param)]
    id_copies = [send(along_task(k), k, ids, every_id.at[t], id_send, id_recv) for k in range(1, n_task)]
    for copy in row_copies + id_copies:
        copy.start()

    def ready(i):
        for copy in fetches(i):
            copy.wait()
        if i + AHEAD < tiles:
            begin(i + AHEAD)

    def reorder(i, w_ref, k, some):
        for q, (first, lane) in some:
            for n, r in enumerate(range(0, emb_dim, ROWS)):
                rows = pl.ds(r, ROWS)
                part = raw[0, 0, rows, :, first:first + lane] if tiles == 1 else raw[i, q, rows]
                wide = part.astype(F32)
                spot = (n + q * (emb_dim // ROWS)) % STAGES * ROWS * PITCH
                for e in range(ROWS):
                    stage[spot + e * PITCH:spot + e * PITCH + groups, :lane] = wide[e]
                for g in range(groups):
                    w_ref[k, g, q, rows, :lane] = stage[pl.ds(spot + g, ROWS, stride=PITCH), :][:, :lane].astype(BF16)

    def add_gram(w_ref, k, some):
        for g in range(groups):
            w = jnp.concatenate([w_ref[k, g, q][:, :lane] for q, (_, lane) in some], axis=1)
            gram[g] += lax.dot_general(w, w, (((1,), (1,)), ((), ())), preferred_element_type=F32)

    gram[...] = jnp.zeros_like(gram)
    steps = list(enumerate(pieces))
    def embed():
        for copy in row_copies + id_copies:
            copy.wait()

        rows_all = table.shape[0] * table.shape[1]
        whole = table[...].reshape(rows_all, emb_dim)
        whole_t = whole.astype(F32).T.astype(BF16)
        per = every_id.shape[2]
        labels = lax.broadcasted_iota(jnp.int32, (rows_all, per), 0)
        embedded_t = []
        for k in range(n_task):
            one_hot = jnp.where(labels == every_id[k], 1.0, 0.0).astype(BF16)
            embedded_t.append(jnp.dot(whole_t, one_hot, preferred_element_type=F32))
            emb_ref[k * per:(k + 1) * per, :] = embedded_t[k].T.astype(BF16)
        emb_t = jnp.concatenate(embedded_t, axis=1)
        turned[...] = emb_t

    for i in range(tiles):
        ready(i)
        w_ref = odd_ref if i % 2 else even_ref
        for n in range(0, blocks, HALF):
            reorder(i, w_ref, i // 2, steps[n:n + HALF])
            add_gram(w_ref, i // 2, steps[n:n + HALF])

    embed()
    count = turned.shape[1]
    width = max(count // SPLIT, LANES)
    halves = [slice(h, h + width) for h in range(0, count, width)]
    first_trip, second_trip = [], []
    for h, lanes in enumerate(halves):
        emb_t = turned[:, lanes]
        emb_low = emb_t.astype(BF16)
        for g in range(groups):
            left = gram[g]
            y = None
            for _ in range(2):
                piece = left.astype(BF16)
                left = left - piece.astype(F32)
                term = jnp.dot(piece, emb_low, preferred_element_type=F32)
                y = term if y is None else y + term
            sums[g:g + 1, lanes] = jnp.sum(y * emb_t, axis=0, keepdims=True)
        first_trip.append([send(along_near(k), (h, k), sums.at[:, lanes], from_near.at[k, :, lanes], a_send, a_recv)
                           for k in range(1, near)])
        for copy in first_trip[h]:
            copy.start()

    for h, lanes in enumerate(halves):
        for copy in first_trip[h]:
            copy.wait()
        total = sums[:, lanes]
        for k in range(1, near):
            total = total + from_near[k, :, lanes]
        part[:, lanes] = total
        second_trip.append([send(along_far(k), (h, k), part.at[:, lanes], from_far.at[k, :, lanes], b_send, b_recv)
                            for k in range(1, high)])
        for copy in second_trip[h]:
            copy.start()

    for h, lanes in enumerate(halves):
        for copy in second_trip[h]:
            copy.wait()
        total = part[:, lanes]
        for k in range(1, high):
            total = total + from_far[k, :, lanes]
        inv_ref[:, lanes] = lax.rsqrt(total / entries + EPSILON)


def second_kernel(keys, width, emb_ref, inv_ref, even_ref, odd_ref, gain_ref, o_hbm, spread, step, sem, *outs):
    tasks = emb_ref.shape[0]
    _, groups, in_tile, _, _ = even_ref.shape
    pieces = pieces_of(o_hbm.shape[2])
    blocks = len(pieces)
    buffers = len({j for j, _, _ in keys})

    def weights(j, g):
        i = j // in_tile
        return (odd_ref if i % 2 else even_ref)[i // 2, g, j % in_tile]

    def widen(c, count):
        for g in range(groups):
            for k in range(c, c + count, LANES):
                row = inv_ref[g:g + 1, k:k + LANES]
                spread[g, k:k + LANES, :] = jnp.broadcast_to(row, (LANES, LANES)).T

    def make(two, c, count):
        made = []
        for g in range(groups):
            w = jnp.concatenate([weights(j, g) for j in two], axis=1)
            made.append(jnp.dot(emb_ref[c:c + count, :], w, preferred_element_type=F32))
        for q, j in enumerate(two):
            lo, lane = pieces[j]
            scaled = []
            for g in range(groups):
                gain = gain_ref[g:g + 1, lo:lo + lane].astype(F32)
                part = made[g][:, q * LANES:q * LANES + lane]
                scaled.append((part * spread[g, c:c + count, :lane] * gain).astype(BF16))
            n = keys.index((j % buffers, c, count))
            first = lo if buffers == 1 else 0
            outs[n][:, :, first:first + lane] = jnp.transpose(jnp.stack(scaled, axis=0), (1, 0, 2))
            if buffers > 1 or j == blocks - 1:
                lanes = slice(None) if buffers == 1 else slice(lo, lo + LANES)
                copy = pltpu.make_async_copy(outs[n], o_hbm.at[c:c + count, :, lanes], sem.at[n])
                copy.start()
                flying.append(copy)

    flying = []
    spans = spans_of(blocks, width) if buffers > 1 else [list(range(blocks))]
    for n, span in enumerate(spans):
        for c, count in cuts_of(tasks, buffers > 1 and n == 0):
            if n == 0:
                widen(c, count)
            for k in range(0, len(span), 2):
                make(span[k:k + 2], c, count)
            pl.semaphore_signal(step, 1)
            pl.semaphore_wait(step, 1)
    for copy in flying:
        copy.wait()


def cuts_of(tasks, fine):
    size = min(tasks, 512)
    cuts = [(c, size) for c in range(0, tasks, size)]
    return [(0, EARLY), (EARLY, size - EARLY)] + cuts[1:] if fine and size > EARLY else cuts


def spans_of(blocks, width):
    cuts = [0, 2] + list(range(2 + width, blocks - 2, width)) + [blocks - 2, blocks]
    cuts = sorted({min(max(cut, 0), blocks) for cut in cuts})
    return [list(range(a, b)) for a, b in zip(cuts, cuts[1:])]


def on_device(n_param, n_task, task_ids, task_table, enc_in, enc_out, generator, gain):
    emb_dim, groups, columns = generator.shape
    table_rows = task_table.shape[0]
    hidden = enc_in.shape[1]
    per = task_ids.shape[0]
    tasks = per * n_task
    entries = columns * n_param * n_task
    blocks = pl.cdiv(columns, LANES)
    buffers = buffers_of(columns)
    tiles = tiles_of(columns)
    in_tile = blocks // tiles
    low = near_factor(n_param)
    near, high = low * n_task, n_param // low
    vmem = pl.BlockSpec(memory_space=pltpu.VMEM)
    hbm = pl.BlockSpec(memory_space=pltpu.HBM)
    dma = pltpu.SemaphoreType.DMA
    limit = SPACE - groups * emb_dim * max(blocks, 2 * in_tile) * LANES * 2 - tasks * emb_dim * 2 - groups * tasks * 4
    even, odd, embedded, inverse = pl.pallas_call(
        functools.partial(first_kernel, n_param, n_task, entries),
        out_shape=(
            pltpu.VMEM((pl.cdiv(tiles, 2), groups, in_tile, emb_dim, LANES), BF16),
            pltpu.VMEM((max(tiles // 2, 1), groups, in_tile, emb_dim, LANES), BF16),
            pltpu.VMEM((tasks, emb_dim), BF16),
            pltpu.VMEM((groups, tasks), F32),
        ),
        in_specs=[hbm] * 5,
        out_specs=(vmem, vmem, vmem, vmem),
        scratch_shapes=[
            pltpu.VMEM((tiles, in_tile, emb_dim, groups, LANES) if tiles > 1 else (1, 1, emb_dim, groups, columns), BF16),
            pltpu.VMEM((STAGES * ROWS * PITCH, LANES), F32),
            pltpu.VMEM((groups, emb_dim, emb_dim), F32),
            pltpu.VMEM((1, per), jnp.int32),
            pltpu.VMEM((table_rows, emb_dim), BF16),
            pltpu.VMEM((emb_dim, hidden), BF16),
            pltpu.VMEM((hidden, emb_dim), BF16),
            pltpu.VMEM((table_rows, emb_dim), BF16),
            pltpu.VMEM((n_param, table_rows, emb_dim), BF16),
            pltpu.VMEM((n_task, 1, per), jnp.int32),
            pltpu.VMEM((emb_dim, tasks), F32),
            pltpu.VMEM((groups, tasks), F32),
            pltpu.VMEM((groups, tasks), F32),
            pltpu.VMEM((near, groups, tasks), F32),
            pltpu.VMEM((high, groups, tasks), F32),
            dma((4,)),
            dma((tiles, in_tile)),
            dma((n_task,)), dma((n_task,)),
            dma((n_param,)), dma((n_param,)),
            dma((SPLIT, near)), dma((SPLIT, near)),
            dma((SPLIT, high)), dma((SPLIT, high)),
        ],
        compiler_params=pltpu.CompilerParams(
            collective_id=0, has_side_effects=True, vmem_limit_bytes=limit),
        name="gather_power",
    )(task_ids.reshape(1, per), task_table, enc_in, enc_out, generator)

    keys = [(j, c, n) for j in range(buffers) for c, n in cuts_of(tasks, buffers > 1 and j < 2)]
    return pl.pallas_call(
        functools.partial(second_kernel, keys, 4),
        out_shape=jax.ShapeDtypeStruct((tasks, groups, columns), BF16),
        in_specs=[vmem] * 5,
        out_specs=hbm,
        scratch_shapes=[
            pltpu.VMEM((groups, tasks, LANES), F32),
            pltpu.SemaphoreType.REGULAR,
            dma((len(keys),)),
            *[pltpu.VMEM((n, groups, columns // buffers), BF16) for _, _, n in keys],
        ],
        compiler_params=pltpu.CompilerParams(vmem_limit_bytes=tasks * groups * LANES * (4 + 2 * blocks) + (3 if buffers > 1 else 12) * MIB),
        name="generate_scale",
    )(embedded, inverse, even, odd, gain)


def solution(mesh):
    placed = (
        P("task"),
        P("param", None),
        P(),
        P(),
        P(None, None, ("param", "task")),
        P(None, ("param", "task")),
    )
    return jax.shard_map(
        functools.partial(on_device, mesh.shape["param"], mesh.shape["task"]),
        mesh=mesh,
        in_specs=placed,
        out_specs=P(None, None, ("param", "task")),
        check_vma=False,
    )
```
